32 devices in a mesh: dom: 32 (over z, y, x, core).
Axes of the slice: x: 2, y: 2, z: 4, core: 2. Of those that a mesh axis runs over, the one named last changes fastest.
Arguments:
- features: bfloat16 [524288, 256], P('dom'), may hold values from -48 to 48, as said below
- w_first: bfloat16 [1280, 256], replicated, may hold values from -0.15625 to 0.15625
- w_second: bfloat16 [1280, 256], replicated, may hold values from -0.15625 to 0.15625
- seed_owner: int32 [9216, 1], P('dom'), may hold values from 0 to 31; in each aligned block of 288 rows (0 to 287, 288 to 575, ...) at most 18 rows name the same one
- seed_row: int32 [9216], P('dom'), may hold values from 0 to 16383
- hop1_owner: int32 [36864, 1], P('dom'), may hold values from 0 to 31; in each aligned block of 1152 rows (0 to 1151, 1152 to 2303, ...) at most 72 rows name the same one
- hop1_row: int32 [36864], P('dom'), may hold values from 0 to 16383
- hop1_rel: int32 [36864], P('dom'), may hold values from 0 to 3
- hop2_owner: int32 [73728, 1], P('dom'), may hold values from 0 to 31; in each aligned block of 2304 rows (0 to 2303, 2304 to 4607, ...) at most 144 rows name the same one
- hop2_row: int32 [73728], P('dom'), may hold values from 0 to 16383
- hop2_rel: int32 [73728], P('dom'), may hold values from 0 to 3
- edge_mask: int32 [4096], P('dom'), may hold values 0 or 1
Outputs:
- edge_loss: float32 [4096], P('dom')
- mean_loss: float32 [], replicated
The draws below stay inside these ranges and needn't reach their ends.
Inputs may be any that keep to these rules, and one draw needn't show every extreme that they name: `features`: standard normal entries; in some draws each row is scaled by a factor up to 10. `seed_owner`: among the rows of one device no owner is named by more than 18 rows; some owner is named by exactly 18 in every draw. `hop1_owner`: among the rows of one device no owner is named by more than 72 rows; some owner is named by exactly 72 in every draw. `hop2_owner`: among the rows of one device no owner is named by more than 144 rows; some owner is named by exactly 144 in every draw.
All inputs are finite; a program needn't handle non-finite values. No bound on the sum of `edge_mask` on one device may be relied on, other than what follows from the above.
Results may differ from the reference program's by a relative error of at most 0.002.
Values may be sent and summed in bfloat16 or wider, within the bound.
A program may use at most 64 MiB of HBM per device.

```python
import math
import jax
import jax.numpy as jnp
import numpy as np
from jax import lax

F = 256
R = 4
NODE_DEV = 16384
POS_DEV = 128
BLOCK = 128
NEG = 32
FAN1 = 4
FAN2 = 2
BLOCKS_DEV = 1
SEED_DEV = 288
H1_DEV = 1152
H2_DEV = 2304
CAP_S = 18
CAP_1 = 72
CAP_2 = 144
NODES = 524288
EDGES = 4096
SEEDS = 9216
H1 = 36864
H2 = 73728
N_DOM = 32


def draw_features(key, part):
    first_key = jax.random.fold_in(key, 0)
    values = jax.random.normal(first_key, (NODES, F), jnp.float32)
    values = jnp.clip(values, -6.0, 6.0)
    return values.astype(jnp.bfloat16)


def place_ends(array, rng, low, high):
    longest = array.shape.index(max(array.shape))
    spots = []
    for shift in (0, 1):
        where = [jax.random.randint(jax.random.fold_in(rng, axis), (), 0, length) for axis, length in enumerate(array.shape)]
        where[longest] = (where[longest] + shift) % array.shape[longest]
        spots.append(tuple(where))
    return array.at[spots[0]].set(low).at[spots[1]].set(high)


def shared_out(rng, own, number, rows, number_of, top, bound, skew):
    sequence = jax.random.permutation(rng, number_of)
    heavy_load, common = portions_of(number_of, rows * top, bound, skew, True), portions_of(number_of, rows * top, bound, skew, False)
    places = jnp.arange(number_of)

    def named(sizes, turn):
        used = int((sizes > 0).sum())
        fixed = max(1, used // 4)
        shifted = fixed + (places - fixed + turn * (used - fixed)) % max(1, number_of - fixed)
        return jnp.zeros((number_of,), jnp.int32).at[sequence[jnp.where(places < fixed, places, shifted)]].set(jnp.asarray(sizes, jnp.int32))

    sizes = jnp.where(number % 4 == 0, named(heavy_load, number // 4), named(common, number - number // 4 - 1))
    mixed = jax.random.permutation(jax.random.fold_in(own, 3), number_of)
    donor, taker = mixed[0:number_of // 2 * 2:2], mixed[1:number_of // 2 * 2:2]
    slack = jnp.minimum(sizes[donor] - 1, bound - sizes[taker]) // 2
    slack = jnp.where((donor == sequence[0]) | (taker == sequence[0]) | (sizes[taker] == 0), 0, jnp.maximum(slack, 0))
    shifted = jax.random.randint(jax.random.fold_in(own, 4), (number_of // 2,), 0, 1 << 20) % (slack + 1)
    sizes = sizes.at[donor].add(-shifted).at[taker].add(shifted)
    members = jnp.searchsorted(jnp.cumsum(sizes), jnp.arange(rows * top), side="right").astype(jnp.int32)
    grid = members.reshape(top, rows).T
    grid = grid[jax.random.permutation(jax.random.fold_in(own, 1), rows)]
    turn = jax.random.randint(jax.random.fold_in(own, 2), (rows, 1), 0, top)
    return jnp.take_along_axis(grid, (jnp.arange(top)[None, :] + turn) % top, axis=1)


def portions_of(amount, total, reach, lean, full):
    loads = [(1 << 20) // math.isqrt(standing ** lean) + 1 for standing in range(1, amount + 1)]
    largest = reach if full else min(reach, max(-(-total // amount), total * loads[0] // sum(loads)))
    least = 1 if total - largest >= amount - 1 else 0
    given, spare = [largest] + [least] * (amount - 1), total - largest - least * (amount - 1)
    while spare > 0:
        movable = [i for i in range(1, amount) if given[i] < largest] or [i for i in range(1, amount) if given[i] < reach]
        mass, remaining = sum([loads[i] for i in movable]), spare
        for i in movable:
            more = min(reach - given[i], max(1, remaining * loads[i] // mass), spare)
            given[i] = given[i] + more
            spare = spare - more
    return np.array(given)


def noise(rng, extent, scale, most, held_as=jnp.bfloat16):
    return jnp.clip(scale * jax.random.normal(rng, extent, jnp.float32), -most, most).astype(held_as)


def setup_inputs(seed: int = 0) -> dict:
    splits = jax.random.split(jax.random.key(seed), 13)
    features = draw_features(jax.random.fold_in(splits[12], 71), 0)
    w_first = noise(splits[1], ((R + 1) * F, F), ((R + 1) * F) ** -0.5, 0.15625)
    w_second = noise(splits[2], ((R + 1) * F, F), ((R + 1) * F) ** -0.5, 0.15625)
    seed_owner_keys = jax.random.split(jax.random.fold_in(splits[3], 1), SEEDS // SEED_DEV)
    seed_owner_turns = jax.random.permutation(jax.random.fold_in(splits[3], 3), SEEDS // SEED_DEV)
    seed_owner = jax.vmap(lambda own, number: shared_out(jax.random.fold_in(splits[3], 2), own, number, SEED_DEV, N_DOM, 1, CAP_S, 2))(seed_owner_keys, seed_owner_turns).reshape((SEEDS, 1))
    seed_row = place_ends(jax.random.randint(splits[4], (SEEDS,), 0, NODE_DEV), jax.random.fold_in(splits[4], 1), 0, NODE_DEV - 1).astype(jnp.int32)
    hop1_owner_keys = jax.random.split(jax.random.fold_in(splits[5], 1), H1 // H1_DEV)
    hop1_owner_turns = jax.random.permutation(jax.random.fold_in(splits[5], 3), H1 // H1_DEV)
    hop1_owner = jax.vmap(lambda own, number: shared_out(jax.random.fold_in(splits[5], 2), own, number, H1_DEV, N_DOM, 1, CAP_1, 2))(hop1_owner_keys, hop1_owner_turns).reshape((H1, 1))
    hop1_row = place_ends(jax.random.randint(splits[6], (H1,), 0, NODE_DEV), jax.random.fold_in(splits[6], 1), 0, NODE_DEV - 1).astype(jnp.int32)
    hop1_rel = place_ends(jax.random.randint(splits[7], (H1,), 0, R), jax.random.fold_in(splits[7], 1), 0, R - 1).astype(jnp.int32)
    hop2_owner_keys = jax.random.split(jax.random.fold_in(splits[8], 1), H2 // H2_DEV)
    hop2_owner_turns = jax.random.permutation(jax.random.fold_in(splits[8], 3), H2 // H2_DEV)
    hop2_owner = jax.vmap(lambda own, number: shared_out(jax.random.fold_in(splits[8], 2), own, number, H2_DEV, N_DOM, 1, CAP_2, 2))(hop2_owner_keys, hop2_owner_turns).reshape((H2, 1))
    hop2_row = place_ends(jax.random.randint(splits[9], (H2,), 0, NODE_DEV), jax.random.fold_in(splits[9], 1), 0, NODE_DEV - 1).astype(jnp.int32)
    hop2_rel = place_ends(jax.random.randint(splits[10], (H2,), 0, R), jax.random.fold_in(splits[10], 1), 0, R - 1).astype(jnp.int32)
    edge_mask = place_ends((jax.random.randint(splits[11], (EDGES,), 0, 4) < 3).astype(jnp.int32), jax.random.fold_in(splits[11], 1), 0, 1)
    return dict(features=features, w_first=w_first, w_second=w_second, seed_owner=seed_owner, seed_row=seed_row, hop1_owner=hop1_owner, hop1_row=hop1_row, hop1_rel=hop1_rel, hop2_owner=hop2_owner, hop2_row=hop2_row, hop2_rel=hop2_rel, edge_mask=edge_mask)


def rgcn_layer(self_rows, neighbours, relations, weights):
    onehot = (relations[..., None] == jnp.arange(R, dtype=jnp.int32)).astype(jnp.float32)
    tallies = jnp.maximum(jnp.sum(onehot, axis=1), 1.0)
    shares = onehot / tallies[:, None, :]
    merged = jnp.einsum('nkr,nkf->nrf', shares, neighbours.astype(jnp.float32)).astype(jnp.bfloat16)
    inputs = jnp.concatenate([self_rows, merged.reshape(self_rows.shape[0], R * F)], axis=1)
    return jnp.dot(inputs, weights, preferred_element_type=jnp.float32)


def edge_scores(second):
    sources = second[:POS_DEV]
    targets = second[POS_DEV:2 * POS_DEV]
    negatives = second[2 * POS_DEV:].reshape(BLOCKS_DEV, NEG, F)
    positive = jnp.sum(sources * targets, axis=1)
    negative = jnp.einsum('bef,bqf->beq', sources.reshape(BLOCKS_DEV, BLOCK, F), negatives,
                          precision=lax.Precision.HIGHEST).reshape(POS_DEV, NEG)
    scores = jnp.concatenate([positive[:, None], negative], axis=1)
    top_score = jnp.max(scores, axis=1, keepdims=True)
    return top_score[:, 0] + jnp.log(jnp.sum(jnp.exp(scores - top_score), axis=1)) - positive


def reference(features, w_first, w_second, seed_owner, seed_row, hop1_owner, hop1_row, hop1_rel,
              hop2_owner, hop2_row, hop2_rel, edge_mask):
    def one_device(pieces):
        s_owner, s_row, a_owner, a_row, a_rel, b_owner, b_row, b_rel = pieces
        x_seed = features[(s_owner * NODE_DEV + s_row).astype(jnp.int32)]
        x_hop1 = features[(a_owner * NODE_DEV + a_row).astype(jnp.int32)]
        x_hop2 = features[(b_owner * NODE_DEV + b_row).astype(jnp.int32)]
        first_hop = jax.nn.relu(rgcn_layer(x_hop1, x_hop2.reshape(H1_DEV, FAN2, F),
                                           b_rel.reshape(H1_DEV, FAN2), w_first)).astype(jnp.bfloat16)
        first_seed = jax.nn.relu(rgcn_layer(x_seed, x_hop1.reshape(SEED_DEV, FAN1, F),
                                            a_rel.reshape(SEED_DEV, FAN1), w_first)).astype(jnp.bfloat16)
        second = rgcn_layer(first_seed, first_hop.reshape(SEED_DEV, FAN1, F),
                            a_rel.reshape(SEED_DEV, FAN1), w_second)
        return edge_scores(second)

    pieces = (seed_owner.reshape(N_DOM, SEED_DEV), seed_row.reshape(N_DOM, SEED_DEV),
              hop1_owner.reshape(N_DOM, H1_DEV), hop1_row.reshape(N_DOM, H1_DEV),
              hop1_rel.reshape(N_DOM, H1_DEV), hop2_owner.reshape(N_DOM, H2_DEV),
              hop2_row.reshape(N_DOM, H2_DEV), hop2_rel.reshape(N_DOM, H2_DEV))
    edge_loss = lax.map(one_device, pieces).reshape(EDGES)
    weights = edge_mask.astype(jnp.float32)
    mean_loss = jnp.sum(weights * edge_loss) / jnp.maximum(jnp.sum(weights), 1.0)
    return edge_loss, mean_loss
```

```python
import jax
import jax.numpy as jnp
import numpy as np
from jax import lax
from jax.sharding import PartitionSpec as P

R = 4
BLOCK = 128
NEG = 32
FAN1 = 4
FAN2 = 2


def bucket_all(owners, rows, group, sets, caps, devices):
    blocks = owners.shape[0] // group
    onehot = owners[:, None] == jnp.arange(devices, dtype=jnp.int32)[None, :]
    hot = onehot.astype(jnp.bfloat16).reshape(blocks, group, devices)
    counter = jnp.arange(group, dtype=jnp.int32)
    earlier = (counter[:, None] > counter[None, :]).astype(jnp.bfloat16)
    prior = jnp.einsum("ij,bjd->bid", earlier, hot, preferred_element_type=jnp.float32)
    totals = jnp.sum(hot.astype(jnp.float32), axis=1)
    carry = []
    start = 0
    for count in sets:
        running = jnp.zeros((devices,), jnp.float32)
        for block in range(start, start + count):
            carry.append(running)
            running = running + totals[block]
        start += count
    prior = prior + jnp.stack(carry)[:, None, :]
    position = jnp.sum(prior * hot.astype(jnp.float32), axis=2).astype(jnp.int32)
    offsets = np.concatenate([[0], np.cumsum(caps)[:-1]])
    offset = jnp.asarray(np.repeat(offsets, sets), jnp.int32)
    capacity = jnp.asarray(np.repeat(np.asarray(caps), sets), jnp.int32)
    slots = owners.reshape(blocks, group) * capacity[:, None] + position
    place = (position + offset[:, None]).reshape(-1)
    width = sum(caps)
    placed = (place[:, None] == jnp.arange(width, dtype=jnp.int32)[None, :]).astype(jnp.bfloat16)
    high = jnp.where(onehot, (rows // 128)[:, None], 0).astype(jnp.bfloat16)
    low = jnp.where(onehot, (rows % 128)[:, None], 0).astype(jnp.bfloat16)
    digits = lax.dot_general(
        jnp.concatenate([high, low], axis=1),
        placed,
        (((0,), (0,)), ((), ())),
        preferred_element_type=jnp.float32,
    )
    requests = (digits[:devices] * 128.0 + digits[devices:]).astype(jnp.int32)
    return slots.reshape(-1), requests


def exchange(requests, features, devices):
    capacity = requests.shape[1]
    located = features[requests.reshape(-1)].reshape(devices, capacity, features.shape[1])
    returned = lax.all_to_all(located, "dom", split_axis=0, concat_axis=0, tiled=True)
    return returned.reshape(devices * capacity, features.shape[1])


def rgcn_layer(self_rows, neighbours, relations, weights):
    width = self_rows.shape[1]
    onehot = (relations[..., None] == jnp.arange(R, dtype=jnp.int32)).astype(jnp.float32)
    tallies = jnp.maximum(jnp.sum(onehot, axis=1), 1.0)
    shares = onehot / tallies[:, None, :]
    merged = shares[:, 0, :, None] * neighbours[:, 0, None, :].astype(jnp.float32)
    for column in range(1, neighbours.shape[1]):
        merged = merged + shares[:, column, :, None] * neighbours[:, column, None, :].astype(
            jnp.float32
        )
    merged = merged.astype(jnp.bfloat16).reshape(self_rows.shape[0], R * width)
    inputs = jnp.concatenate([self_rows, merged], axis=1)
    return jnp.dot(inputs, weights, preferred_element_type=jnp.float32)


def shards(
    features,
    w_first,
    w_second,
    seed_owner,
    seed_row,
    hop1_owner,
    hop1_row,
    hop1_rel,
    hop2_owner,
    hop2_row,
    hop2_rel,
    edge_mask,
):
    devices = lax.axis_size("dom")
    width = features.shape[1]
    seed_count = seed_row.shape[0]
    first_count = hop1_row.shape[0]
    positives = edge_mask.shape[0]
    blocks = positives // BLOCK
    second_count = hop2_row.shape[0]
    caps = [
        (2 * length + devices - 1) // devices for length in (second_count, first_count, seed_count)
    ]
    owners = jnp.concatenate([hop2_owner[:, 0], hop1_owner[:, 0], seed_owner[:, 0]])
    rows = jnp.concatenate([hop2_row, hop1_row, seed_row])
    sets = (second_count // seed_count, first_count // seed_count, 1)
    slots, requests = bucket_all(owners, rows, seed_count, sets, caps, devices)
    arrived = lax.all_to_all(requests, "dom", split_axis=0, concat_axis=0, tiled=True)
    near = caps[0]
    middle = caps[0] + caps[1]
    got_hop2 = exchange(arrived[:, :near], features, devices)
    got_hop1 = exchange(arrived[:, near:middle], features, devices)
    got_seed = exchange(arrived[:, middle:], features, devices)
    x_hop2 = got_hop2[slots[:second_count]]
    x_hop1 = got_hop1[slots[second_count : second_count + first_count]]
    x_seed = got_seed[slots[second_count + first_count :]]
    first_hop = jax.nn.relu(
        rgcn_layer(
            x_hop1,
            x_hop2.reshape(first_count, FAN2, width),
            hop2_rel.reshape(first_count, FAN2),
            w_first,
        )
    ).astype(jnp.bfloat16)
    first_seed = jax.nn.relu(
        rgcn_layer(
            x_seed,
            x_hop1.reshape(seed_count, FAN1, width),
            hop1_rel.reshape(seed_count, FAN1),
            w_first,
        )
    ).astype(jnp.bfloat16)
    second = rgcn_layer(
        first_seed,
        first_hop.reshape(seed_count, FAN1, width),
        hop1_rel.reshape(seed_count, FAN1),
        w_second,
    )
    sources = second[:positives]
    targets = second[positives : 2 * positives]
    negatives = second[2 * positives :].reshape(blocks, NEG, width)
    positive = jnp.sum(sources * targets, axis=1)
    negative = jnp.einsum(
        "bef,bqf->beq",
        sources.reshape(blocks, BLOCK, width),
        negatives,
        precision=lax.Precision.HIGHEST,
    ).reshape(positives, NEG)
    scores = jnp.concatenate([positive[:, None], negative], axis=1)
    top_score = jnp.max(scores, axis=1, keepdims=True)
    edge_loss = top_score[:, 0] + jnp.log(jnp.sum(jnp.exp(scores - top_score), axis=1)) - positive
    weights = edge_mask.astype(jnp.float32)
    sums = jnp.stack([jnp.sum(weights * edge_loss), jnp.sum(weights)])
    loss_total, edge_total = jnp.sum(lax.all_gather(sums, "dom"), axis=0)
    mean_loss = loss_total / jnp.maximum(edge_total, 1.0)
    return (edge_loss, mean_loss)


def solution(mesh):
    placed = (
        P("dom", None),
        P(),
        P(),
        P("dom", None),
        P("dom"),
        P("dom", None),
        P("dom"),
        P("dom"),
        P("dom", None),
        P("dom"),
        P("dom"),
        P("dom"),
    )
    return jax.shard_map(
        shards, mesh=mesh, in_specs=placed, out_specs=(P("dom"), P()), check_vma=False
    )
```

```python
import functools

import jax
import jax.numpy as jnp
import numpy as np
from jax import lax
from jax.experimental import pallas as pl
from jax.experimental.pallas import tpu as pltpu
from jax.sharding import PartitionSpec as P

MESH = pl.DeviceIdType.MESH
HOP = 11
PIECE = 96
LANES = 128

R = 4
BLOCK = 128
NEG = 32
FAN1 = 4
FAN2 = 2


def round_up(value, multiple):
    return (value + multiple - 1) // multiple * multiple


def unroll_of(count):
    return max(step for step in range(1, 25) if count % step == 0)


def bucket_all(owners, rows, group, sets, caps, bases, strides, devices):
    blocks = owners.shape[0] // group
    onehot = owners[:, None] == jnp.arange(devices, dtype=jnp.int32)[None, :]
    hot = onehot.astype(jnp.bfloat16).reshape(blocks, group, devices)
    counter = jnp.arange(group, dtype=jnp.int32)
    earlier = (counter[:, None] > counter[None, :]).astype(jnp.bfloat16)
    prior = jnp.einsum("ij,bjd->bid", earlier, hot, preferred_element_type=jnp.float32)
    totals = jnp.sum(hot.astype(jnp.float32), axis=1)
    carry = []
    start = 0
    for count in sets:
        running = jnp.zeros((devices,), jnp.float32)
        for block in range(start, start + count):
            carry.append(running)
            running = running + totals[block]
        start += count
    prior = prior + jnp.stack(carry)[:, None, :]
    position = jnp.sum(prior * hot.astype(jnp.float32), axis=2).astype(jnp.int32)
    offsets = np.concatenate([[0], np.cumsum(caps)[:-1]])
    offset = jnp.asarray(np.repeat(offsets, sets), jnp.int32)
    base = jnp.asarray(np.repeat(np.asarray(bases), sets), jnp.int32)
    stride = jnp.asarray(np.repeat(np.asarray(strides), sets), jnp.int32)
    slots = owners.reshape(blocks, group) * stride[:, None] + base[:, None] + position
    place = (position + offset[:, None]).reshape(-1)
    width = round_up(sum(caps), LANES)
    placed = (place[:, None] == jnp.arange(width, dtype=jnp.int32)[None, :]).astype(jnp.bfloat16)
    high = jnp.where(onehot, (rows // 128)[:, None], 0).astype(jnp.bfloat16)
    low = jnp.where(onehot, (rows % 128)[:, None], 0).astype(jnp.bfloat16)
    digits = lax.dot_general(
        jnp.concatenate([high, low], axis=1),
        placed,
        (((0,), (0,)), ((), ())),
        preferred_element_type=jnp.float32,
    )
    requests = (digits[:devices] * 128.0 + digits[devices:]).astype(jnp.int32)
    return slots.reshape(-1), requests


def greet(devices, me):
    barrier = pltpu.get_barrier_semaphore()

    def hail(step, carry):
        other = lax.rem(me + step, devices)
        pl.semaphore_signal(barrier, inc=1, device_id=(other,), device_id_type=MESH)
        return carry

    lax.fori_loop(1, devices, hail, 0)
    pl.semaphore_wait(barrier, devices - 1)


def gather_rows(table, index_of, count, staging):
    step = unroll_of(count)

    def some(turn, carry):
        for lane in range(step):
            place = turn * step + lane
            staging[pl.ds(place, 1), :] = table[pl.ds(index_of(place), 1), :]
        return carry

    lax.fori_loop(0, count // step, some, 0)


def fetch_kernel(
    devices,
    caps,
    strides,
    requests,
    slots,
    features,
    far_out,
    near_out,
    table_half,
    table,
    arrived,
    wanted,
    far_send,
    near_send,
    far_recv,
    near_recv,
    far_table,
    near_table,
    staging,
    load_sem,
    small_sem,
    ask_send,
    ask_recv,
    far_send_sem,
    far_recv_sem,
    near_send_sem,
    near_recv_sem,
):
    me = lax.axis_index("dom")
    far_cap, near_cap = caps
    load = pltpu.make_async_copy(features, table_half, load_sem)
    load.start()
    greet(devices, me)

    def ask(turn, carry):
        other = lax.rem(me + turn * HOP, devices)
        pltpu.make_async_remote_copy(
            src_ref=requests.at[other],
            dst_ref=arrived.at[me],
            send_sem=ask_send,
            recv_sem=ask_recv,
            device_id=(other,),
            device_id_type=MESH,
        ).start()
        return carry

    lax.fori_loop(1, devices, ask, 0)
    own = pltpu.make_async_copy(requests.at[me], arrived.at[me], small_sem)
    own.start()
    load.wait()
    nodes = table.shape[0]
    chunk = nodes // 32

    def widen(turn, carry):
        where = pl.ds(pl.multiple_of(turn * chunk, chunk), chunk)
        table[where, :] = table_half[where, :].astype(jnp.float32)
        return carry

    lax.fori_loop(0, 32, widen, 0)
    own.wait()
    others = pl.ds(0, devices - 1)
    pltpu.make_async_copy(requests.at[others], arrived.at[others], ask_send).wait()
    pltpu.make_async_copy(requests.at[others], arrived.at[others], ask_recv).wait()
    move = pltpu.make_async_copy(arrived, wanted, small_sem)
    move.start()
    move.wait()

    def serve(first, cap, send, recv, send_sem, recv_sem):
        def pick(other):
            gather_rows(table, lambda place: wanted[other, 0, first + place], cap, staging)
            return staging[pl.ds(0, cap), :].astype(jnp.bfloat16)

        def one(turn, carry):
            other = lax.rem(me + turn * HOP, devices)
            send[other] = pick(other)
            pltpu.make_async_remote_copy(
                src_ref=send.at[other],
                dst_ref=recv.at[me],
                send_sem=send_sem,
                recv_sem=recv_sem,
                device_id=(other,),
                device_id_type=MESH,
            ).start()
            return carry

        lax.fori_loop(1, devices, one, 0)
        recv[me] = pick(me)

    serve(0, far_cap, far_send, far_recv, far_send_sem, far_recv_sem)
    serve(far_cap, near_cap, near_send, near_recv, near_send_sem, near_recv_sem)

    def settle(send, recv, recv_sem, cap, stride, wide, offset, out):
        pltpu.make_async_copy(send.at[others], recv.at[others], recv_sem).wait()

        def spread(source, carry):
            where = pl.ds(pl.multiple_of(source * stride, 8), cap)
            wide[where, :] = recv[source].astype(jnp.float32)
            return carry

        lax.fori_loop(0, devices, spread, 0)

        def piece(turn, carry):
            start = pl.multiple_of(turn * PIECE, PIECE)
            gather_rows(wide, lambda place: slots[offset + start + place], PIECE, staging)
            out[pl.ds(start, PIECE), :] = staging[pl.ds(0, PIECE), :].astype(jnp.bfloat16)
            return carry

        lax.fori_loop(0, out.shape[0] // PIECE, piece, 0)

    settle(far_send, far_recv, far_recv_sem, far_cap, strides[0], far_table, 0, far_out)
    settle(
        near_send,
        near_recv,
        near_recv_sem,
        near_cap,
        strides[1],
        near_table,
        far_out.shape[0],
        near_out,
    )
    pltpu.make_async_copy(far_send.at[others], far_recv.at[others], far_send_sem).wait()
    pltpu.make_async_copy(near_send.at[others], near_recv.at[others], near_send_sem).wait()


def fetch(requests, slots, features, caps, strides, counts, devices):
    nodes, width = features.shape
    far_cap, near_cap = caps
    asked = requests.shape[1]
    half, full = jnp.bfloat16, jnp.float32
    vmem = pl.BlockSpec(memory_space=pltpu.VMEM)
    return pl.pallas_call(
        functools.partial(fetch_kernel, devices, caps, strides),
        out_shape=[jax.ShapeDtypeStruct((count, width), half) for count in counts],
        in_specs=[
            vmem,
            pl.BlockSpec(memory_space=pltpu.SMEM),
            pl.BlockSpec(memory_space=pl.ANY),
        ],
        out_specs=[vmem, vmem],
        scratch_shapes=[
            pltpu.VMEM((nodes, width), half),
            pltpu.VMEM((nodes, width), full),
            pltpu.VMEM((devices, 1, asked), jnp.int32),
            pltpu.SMEM((devices, 1, asked), jnp.int32),
            pltpu.VMEM((devices, far_cap, width), half),
            pltpu.VMEM((devices, near_cap, width), half),
            pltpu.VMEM((devices, far_cap, width), half),
            pltpu.VMEM((devices, near_cap, width), half),
            pltpu.VMEM((devices * strides[0], width), full),
            pltpu.VMEM((devices * strides[1], width), full),
            pltpu.VMEM((round_up(max(far_cap, near_cap, PIECE), 8), width), full),
        ]
        + [pltpu.SemaphoreType.DMA(())] * 8,
        compiler_params=pltpu.CompilerParams(
            collective_id=0, has_side_effects=True, vmem_limit_bytes=60 * 1024 * 1024
        ),
        name="fetch",
    )(requests.reshape(devices, 1, asked), slots, features)


def total_kernel(devices, part, out, seen, send_sem, recv_sem):
    me = lax.axis_index("dom")
    greet(devices, me)

    def tell(turn, carry):
        other = lax.rem(me + turn * HOP, devices)
        pltpu.make_async_remote_copy(
            src_ref=part,
            dst_ref=seen.at[me],
            send_sem=send_sem,
            recv_sem=recv_sem,
            device_id=(other,),
            device_id_type=MESH,
        ).start()
        return carry

    lax.fori_loop(1, devices, tell, 0)
    seen[me] = part[...]
    others = pl.ds(0, devices - 1)
    pltpu.make_async_copy(seen.at[others], seen.at[others], recv_sem).wait()
    pltpu.make_async_copy(seen.at[others], seen.at[others], send_sem).wait()
    out[...] = jnp.sum(seen[...], axis=0)


def total_over(part, devices):
    return pl.pallas_call(
        functools.partial(total_kernel, devices),
        out_shape=jax.ShapeDtypeStruct(part.shape, part.dtype),
        in_specs=[pl.BlockSpec(memory_space=pltpu.VMEM)],
        out_specs=pl.BlockSpec(memory_space=pltpu.VMEM),
        scratch_shapes=[
            pltpu.VMEM((devices,) + part.shape, part.dtype),
            pltpu.SemaphoreType.DMA(()),
            pltpu.SemaphoreType.DMA(()),
        ],
        compiler_params=pltpu.CompilerParams(collective_id=1, has_side_effects=True),
        name="total",
    )(part)


def rgcn_layer(self_rows, neighbours, relations, weights):
    hot = [
        (relation[:, None] == jnp.arange(R, dtype=jnp.int32)[None, :]).astype(jnp.float32)
        for relation in relations
    ]
    tallies = jnp.maximum(sum(hot[1:], hot[0]), 1.0)
    wide = [neighbour.astype(jnp.float32) for neighbour in neighbours]
    means = []
    for kind in range(R):
        mean = (hot[0][:, kind] / tallies[:, kind])[:, None] * wide[0]
        for one, rows in zip(hot[1:], wide[1:]):
            mean = mean + (one[:, kind] / tallies[:, kind])[:, None] * rows
        means.append(mean.astype(jnp.bfloat16))
    inputs = jnp.concatenate([self_rows] + means, axis=1)
    return jnp.dot(inputs, weights, preferred_element_type=jnp.float32)


def shards(
    features,
    w_first,
    w_second,
    seed_owner,
    seed_row,
    hop1_owner,
    hop1_row,
    hop1_rel,
    hop2_owner,
    hop2_row,
    hop2_rel,
    edge_mask,
):
    devices = lax.axis_size("dom")
    width = features.shape[1]
    seed_count = seed_row.shape[0]
    first_count = hop1_row.shape[0]
    positives = edge_mask.shape[0]
    blocks = positives // BLOCK
    second_count = hop2_row.shape[0]
    caps = [
        (2 * length + devices - 1) // devices for length in (second_count, first_count, seed_count)
    ]
    near_cap = caps[1] + caps[2]
    strides = (round_up(caps[0], 8), round_up(near_cap, 8))

    def turned(values, fan):
        return values.reshape(-1, fan).T

    def hop2_order(values):
        return turned(values, FAN2).reshape(FAN2, seed_count, FAN1).swapaxes(1, 2).reshape(-1)

    def hop1_order(values):
        return turned(values, FAN1).reshape(-1)

    owners = jnp.concatenate(
        [hop2_order(hop2_owner[:, 0]), hop1_order(hop1_owner[:, 0]), seed_owner[:, 0]]
    )
    rows = jnp.concatenate([hop2_order(hop2_row), hop1_order(hop1_row), seed_row])
    sets = (second_count // seed_count, first_count // seed_count, 1)
    slots, requests = bucket_all(
        owners,
        rows,
        seed_count,
        sets,
        caps,
        (0, 0, caps[1]),
        (strides[0], strides[1], strides[1]),
        devices,
    )
    x_hop2, x_near = fetch(
        requests,
        slots,
        features,
        (caps[0], near_cap),
        strides,
        (second_count, first_count + seed_count),
        devices,
    )
    x_hop1 = x_near[:first_count]
    x_seed = x_near[first_count:]
    hop2_kinds = hop2_order(hop2_rel).reshape(FAN2, first_count)
    hop1_kinds = hop1_order(hop1_rel).reshape(FAN1, seed_count)
    first_hop = jax.nn.relu(
        rgcn_layer(
            x_hop1,
            [x_hop2[k * first_count : (k + 1) * first_count] for k in range(FAN2)],
            [hop2_kinds[k] for k in range(FAN2)],
            w_first,
        )
    ).astype(jnp.bfloat16)

    def by_seed(values):
        return [values[k * seed_count : (k + 1) * seed_count] for k in range(FAN1)]

    seed_kinds = [hop1_kinds[k] for k in range(FAN1)]
    first_seed = jax.nn.relu(
        rgcn_layer(x_seed, by_seed(x_hop1), seed_kinds, w_first)
    ).astype(jnp.bfloat16)
    second = rgcn_layer(first_seed, by_seed(first_hop), seed_kinds, w_second)
    sources = second[:positives]
    targets = second[positives : 2 * positives]
    negatives = second[2 * positives :].reshape(blocks, NEG, width)
    positive = jnp.sum(sources * targets, axis=1)
    negative = jnp.einsum(
        "bef,bqf->beq",
        sources.reshape(blocks, BLOCK, width),
        negatives,
        precision=lax.Precision.HIGHEST,
    ).reshape(positives, NEG)
    scores = jnp.concatenate([positive[:, None], negative], axis=1)
    top_score = jnp.max(scores, axis=1, keepdims=True)
    edge_loss = top_score[:, 0] + jnp.log(jnp.sum(jnp.exp(scores - top_score), axis=1)) - positive
    weights = edge_mask.astype(jnp.float32)
    lane = jnp.arange(LANES, dtype=jnp.int32)[None, :]
    part = jnp.where(lane == 0, jnp.sum(weights * edge_loss), 0.0)
    part = jnp.where(lane == 1, jnp.sum(weights), part)
    total = total_over(part, devices)
    loss_total, edge_total = total[0, 0], total[0, 1]
    mean_loss = loss_total / jnp.maximum(edge_total, 1.0)
    return (edge_loss, mean_loss)


def solution(mesh):
    placed = (
        P("dom", None),
        P(),
        P(),
        P("dom", None),
        P("dom"),
        P("dom", None),
        P("dom"),
        P("dom"),
        P("dom", None),
        P("dom"),
        P("dom"),
        P("dom"),
    )
    return jax.shard_map(
        shards, mesh=mesh, in_specs=placed, out_specs=(P("dom"), P()), check_vma=False
    )
```

```python
import functools

import jax
import jax.numpy as jnp
import numpy as np
from jax import lax
from jax.experimental import pallas as pl
from jax.experimental.pallas import tpu as pltpu
from jax.sharding import PartitionSpec as P

MESH = pl.DeviceIdType.MESH
HOP = 11
PIECE = 96
LANES = 128

R = 4
BLOCK = 128
NEG = 32
FAN1 = 4
FAN2 = 2


def round_up(value, multiple):
    return (value + multiple - 1) // multiple * multiple


def unroll_of(count):
    return max(step for step in range(1, 25) if count % step == 0)


def bucket_all(owners, rows, group, sets, caps, bases, strides, devices):
    blocks = owners.shape[0] // group
    onehot = owners[:, None] == jnp.arange(devices, dtype=jnp.int32)[None, :]
    hot = onehot.astype(jnp.bfloat16).reshape(blocks, group, devices)
    counter = jnp.arange(group, dtype=jnp.int32)
    earlier = (counter[:, None] > counter[None, :]).astype(jnp.bfloat16)
    prior = jnp.einsum("ij,bjd->bid", earlier, hot, preferred_element_type=jnp.float32)
    totals = jnp.sum(hot.astype(jnp.float32), axis=1)
    carry = []
    start = 0
    for count in sets:
        running = jnp.zeros((devices,), jnp.float32)
        for block in range(start, start + count):
            carry.append(running)
            running = running + totals[block]
        start += count
    prior = prior + jnp.stack(carry)[:, None, :]
    position = jnp.sum(prior * hot.astype(jnp.float32), axis=2).astype(jnp.int32)
    offsets = np.concatenate([[0], np.cumsum(caps)[:-1]])
    offset = jnp.asarray(np.repeat(offsets, sets), jnp.int32)
    base = jnp.asarray(np.repeat(np.asarray(bases), sets), jnp.int32)
    stride = jnp.asarray(np.repeat(np.asarray(strides), sets), jnp.int32)
    slots = owners.reshape(blocks, group) * stride[:, None] + base[:, None] + position
    place = (position + offset[:, None]).reshape(-1)
    width = round_up(sum(caps), LANES)
    placed = (place[:, None] == jnp.arange(width, dtype=jnp.int32)[None, :]).astype(jnp.bfloat16)
    high = jnp.where(onehot, (rows // 128)[:, None], 0).astype(jnp.bfloat16)
    low = jnp.where(onehot, (rows % 128)[:, None], 0).astype(jnp.bfloat16)
    digits = lax.dot_general(
        jnp.concatenate([high, low], axis=1),
        placed,
        (((0,), (0,)), ((), ())),
        preferred_element_type=jnp.float32,
    )
    requests = (digits[:devices] * 128.0 + digits[devices:]).astype(jnp.int32)
    return slots.reshape(-1), requests


def greet(devices, me):
    barrier = pltpu.get_barrier_semaphore()

    def hail(step, carry):
        other = lax.rem(me + step, devices)
        pl.semaphore_signal(barrier, inc=1, device_id=(other,), device_id_type=MESH)
        return carry

    lax.fori_loop(1, devices, hail, 0)
    pl.semaphore_wait(barrier, devices - 1)


def gather_rows(table, index_of, count, staging):
    step = unroll_of(count)

    def some(turn, carry):
        for lane in range(step):
            place = turn * step + lane
            staging[pl.ds(place, 1), :] = table[pl.ds(index_of(place), 1), :]
        return carry

    lax.fori_loop(0, count // step, some, 0)


def fetch_kernel(
    devices,
    caps,
    strides,
    counts,
    requests,
    slots,
    features,
    w_first,
    w_second,
    far_kinds,
    near_kinds,
    mask,
    loss_out,
    mean_out,
    table_half,
    table,
    arrived,
    wanted,
    far_send,
    near_send,
    far_recv,
    near_recv,
    far_table,
    near_table,
    staging,
    partial,
    near_rows,
    first_hop,
    first_seed,
    second,
    part,
    seen,
    load_sem,
    small_sem,
    ask_send,
    ask_recv,
    far_send_sem,
    far_recv_sem,
    near_send_sem,
    near_recv_sem,
    tell_send,
    tell_recv,
):
    me = lax.axis_index("dom")
    far_count, first_count, seed_count = counts
    width = table.shape[1]
    far_cap, near_cap = caps
    load = pltpu.make_async_copy(features, table_half, load_sem)
    load.start()
    greet(devices, me)

    def ask(turn, carry):
        other = lax.rem(me + turn * HOP, devices)
        pltpu.make_async_remote_copy(
            src_ref=requests.at[other],
            dst_ref=arrived.at[me],
            send_sem=ask_send,
            recv_sem=ask_recv,
            device_id=(other,),
            device_id_type=MESH,
        ).start()
        return carry

    lax.fori_loop(1, devices, ask, 0)
    own = pltpu.make_async_copy(requests.at[me], arrived.at[me], small_sem)
    own.start()
    load.wait()
    nodes = table.shape[0]
    chunk = nodes // 32

    def widen(turn, carry):
        where = pl.ds(pl.multiple_of(turn * chunk, chunk), chunk)
        table[where, :] = table_half[where, :].astype(jnp.float32)
        return carry

    lax.fori_loop(0, 32, widen, 0)
    own.wait()
    others = pl.ds(0, devices - 1)
    pltpu.make_async_copy(requests.at[others], arrived.at[others], ask_send).wait()
    pltpu.make_async_copy(requests.at[others], arrived.at[others], ask_recv).wait()
    move = pltpu.make_async_copy(arrived, wanted, small_sem)
    move.start()
    move.wait()

    def serve(first, cap, send, recv, send_sem, recv_sem):
        def pick(other):
            gather_rows(table, lambda place: wanted[other, 0, first + place], cap, staging)
            return staging[pl.ds(0, cap), :].astype(jnp.bfloat16)

        def one(turn, carry):
            other = lax.rem(me + turn * HOP, devices)
            send[other] = pick(other)
            pltpu.make_async_remote_copy(
                src_ref=send.at[other],
                dst_ref=recv.at[me],
                send_sem=send_sem,
                recv_sem=recv_sem,
                device_id=(other,),
                device_id_type=MESH,
            ).start()
            return carry

        lax.fori_loop(1, devices, one, 0)
        recv[me] = pick(me)

    serve(0, far_cap, far_send, far_recv, far_send_sem, far_recv_sem)
    serve(far_cap, near_cap, near_send, near_recv, near_send_sem, near_recv_sem)

    def settle(send, recv, recv_sem, cap, stride, wide):
        pltpu.make_async_copy(send.at[others], recv.at[others], recv_sem).wait()

        def spread(source, carry):
            where = pl.ds(pl.multiple_of(source * stride, 8), cap)
            wide[where, :] = recv[source].astype(jnp.float32)
            return carry

        lax.fori_loop(0, devices, spread, 0)

    def weighed(values, kinds, weights):
        fan = len(values)
        hot = [
            [(kinds[:, k : k + 1] == kind).astype(jnp.float32) for k in range(fan)]
            for kind in range(R)
        ]
        result = None
        for kind in range(R):
            share = 1.0 / jnp.maximum(sum(hot[kind][1:], hot[kind][0]), 1.0)
            mean = (hot[kind][0] * share) * values[0]
            for k in range(1, fan):
                mean = mean + (hot[kind][k] * share) * values[k]
            term = jnp.dot(
                mean.astype(jnp.bfloat16),
                weights[(kind + 1) * width : (kind + 2) * width, :],
                preferred_element_type=jnp.float32,
            )
            result = term if result is None else result + term
        return result

    def itself(values, weights):
        return jnp.dot(
            values.astype(jnp.bfloat16), weights[:width, :], preferred_element_type=jnp.float32
        )

    settle(far_send, far_recv, far_recv_sem, far_cap, strides[0], far_table)

    def far_piece(turn, carry):
        start = pl.multiple_of(turn * PIECE, PIECE)
        values = []
        for k in range(FAN2):
            gather_rows(
                far_table, lambda place: slots[k * first_count + start + place], PIECE, staging
            )
            values.append(staging[pl.ds(0, PIECE), :])
        where = pl.ds(start, PIECE)
        partial[where, :] = weighed(values, far_kinds[where, :], w_first)
        return carry

    lax.fori_loop(0, first_count // PIECE, far_piece, 0)
    settle(near_send, near_recv, near_recv_sem, near_cap, strides[1], near_table)
    gather_rows(
        near_table, lambda place: slots[far_count + place], first_count + seed_count, near_rows
    )

    def hop_piece(turn, carry):
        where = pl.ds(pl.multiple_of(turn * PIECE, PIECE), PIECE)
        layer = itself(near_rows[where, :], w_first) + partial[where, :]
        rounded = jnp.maximum(layer, 0.0).astype(jnp.bfloat16)
        first_hop[where, :] = rounded.astype(jnp.float32)
        return carry

    lax.fori_loop(0, first_count // PIECE, hop_piece, 0)

    def seed_layer(start, own_rows, own_start, rows, weights):
        where = pl.ds(start, PIECE)
        values = [
            rows[pl.ds(pl.multiple_of(k * seed_count + start, PIECE), PIECE), :]
            for k in range(FAN1)
        ]
        own_where = pl.ds(pl.multiple_of(own_start + start, PIECE), PIECE)
        return itself(own_rows[own_where, :], weights) + weighed(
            values, near_kinds[where, :], weights
        )

    def seed_piece(turn, carry):
        start = pl.multiple_of(turn * PIECE, PIECE)
        where = pl.ds(start, PIECE)
        layer = seed_layer(start, near_rows, first_count, near_rows, w_first)
        first_seed[where, :] = jnp.maximum(layer, 0.0).astype(jnp.bfloat16).astype(jnp.float32)
        second[where, :] = seed_layer(start, first_seed, 0, first_hop, w_second)
        return carry

    lax.fori_loop(0, seed_count // PIECE, seed_piece, 0)

    positives = mask.shape[0]
    loss_sum = jnp.zeros((1, 1), jnp.float32)
    edge_sum = jnp.zeros((1, 1), jnp.float32)
    for block in range(positives // BLOCK):
        span = slice(block * BLOCK, (block + 1) * BLOCK)
        sources = second[span, :]
        targets = second[positives + block * BLOCK : positives + (block + 1) * BLOCK, :]
        first_neg = 2 * positives + block * NEG
        negatives = second[first_neg : first_neg + NEG, :]
        positive = jnp.sum(sources * targets, axis=1, keepdims=True)
        negative = lax.dot_general(
            sources,
            negatives,
            (((1,), (1,)), ((), ())),
            precision=lax.Precision.HIGHEST,
            preferred_element_type=jnp.float32,
        )
        top_score = jnp.maximum(positive, jnp.max(negative, axis=1, keepdims=True))
        spread_sum = jnp.exp(positive - top_score) + jnp.sum(
            jnp.exp(negative - top_score), axis=1, keepdims=True
        )
        edge_loss = top_score + jnp.log(spread_sum) - positive
        loss_out[span, :] = edge_loss
        counted = mask[span, :].astype(jnp.float32)
        loss_sum = loss_sum + jnp.sum(counted * edge_loss, axis=0, keepdims=True)
        edge_sum = edge_sum + jnp.sum(counted, axis=0, keepdims=True)
    lane = lax.broadcasted_iota(jnp.int32, (1, LANES), 1)
    part[...] = jnp.where(lane == 0, loss_sum, jnp.where(lane == 1, edge_sum, 0.0))

    def tell(turn, carry):
        other = lax.rem(me + turn * HOP, devices)
        pltpu.make_async_remote_copy(
            src_ref=part,
            dst_ref=seen.at[me],
            send_sem=tell_send,
            recv_sem=tell_recv,
            device_id=(other,),
            device_id_type=MESH,
        ).start()
        return carry

    lax.fori_loop(1, devices, tell, 0)
    seen[me] = part[...]
    pltpu.make_async_copy(far_send.at[others], far_recv.at[others], far_send_sem).wait()
    pltpu.make_async_copy(near_send.at[others], near_recv.at[others], near_send_sem).wait()
    pltpu.make_async_copy(seen.at[others], seen.at[others], tell_recv).wait()
    pltpu.make_async_copy(seen.at[others], seen.at[others], tell_send).wait()
    total = jnp.sum(seen[...], axis=0)
    mean_out[...] = total[:, 0:1] / jnp.maximum(total[:, 1:2], 1.0)


def fetch(
    requests, slots, features, w_first, w_second, kinds, mask, caps, strides, counts, devices
):
    nodes, width = features.shape
    far_cap, near_cap = caps
    asked = requests.shape[1]
    half, full = jnp.bfloat16, jnp.float32
    vmem = pl.BlockSpec(memory_space=pltpu.VMEM)
    return pl.pallas_call(
        functools.partial(fetch_kernel, devices, caps, strides, counts),
        out_shape=[
            jax.ShapeDtypeStruct(mask.shape, full),
            jax.ShapeDtypeStruct((1, 1), full),
        ],
        in_specs=[
            vmem,
            pl.BlockSpec(memory_space=pltpu.SMEM),
            pl.BlockSpec(memory_space=pl.ANY),
        ]
        + [vmem] * 5,
        out_specs=[vmem, vmem],
        scratch_shapes=[
            pltpu.VMEM((nodes, width), half),
            pltpu.VMEM((nodes, width), full),
            pltpu.VMEM((devices, 1, asked), jnp.int32),
            pltpu.SMEM((devices, 1, asked), jnp.int32),
            pltpu.VMEM((devices, far_cap, width), half),
            pltpu.VMEM((devices, near_cap, width), half),
            pltpu.VMEM((devices, far_cap, width), half),
            pltpu.VMEM((devices, near_cap, width), half),
            pltpu.VMEM((devices * strides[0], width), full),
            pltpu.VMEM((devices * strides[1], width), full),
            pltpu.VMEM((round_up(max(far_cap, near_cap, PIECE), 8), width), full),
            pltpu.VMEM((counts[1], width), full),
            pltpu.VMEM((counts[1] + counts[2], width), full),
            pltpu.VMEM((counts[1], width), full),
            pltpu.VMEM((counts[2], width), full),
            pltpu.VMEM((counts[2], width), full),
            pltpu.VMEM((1, LANES), full),
            pltpu.VMEM((devices, 1, LANES), full),
        ]
        + [pltpu.SemaphoreType.DMA(())] * 10,
        compiler_params=pltpu.CompilerParams(
            collective_id=0, has_side_effects=True, vmem_limit_bytes=60 * 1024 * 1024
        ),
        name="fetch",
    )(
        requests.reshape(devices, 1, asked),
        slots,
        features,
        w_first,
        w_second,
        kinds[0],
        kinds[1],
        mask,
    )


def shards(
    features,
    w_first,
    w_second,
    seed_owner,
    seed_row,
    hop1_owner,
    hop1_row,
    hop1_rel,
    hop2_owner,
    hop2_row,
    hop2_rel,
    edge_mask,
):
    devices = lax.axis_size("dom")
    seed_count = seed_row.shape[0]
    first_count = hop1_row.shape[0]
    second_count = hop2_row.shape[0]
    caps = [
        (2 * length + devices - 1) // devices for length in (second_count, first_count, seed_count)
    ]
    near_cap = caps[1] + caps[2]
    strides = (round_up(caps[0], 8), round_up(near_cap, 8))

    def turned(values, fan):
        return values.reshape(-1, fan).T

    def hop2_order(values):
        return turned(values, FAN2).reshape(FAN2, seed_count, FAN1).swapaxes(1, 2).reshape(-1)

    def hop1_order(values):
        return turned(values, FAN1).reshape(-1)

    owners = jnp.concatenate(
        [hop2_order(hop2_owner[:, 0]), hop1_order(hop1_owner[:, 0]), seed_owner[:, 0]]
    )
    rows = jnp.concatenate([hop2_order(hop2_row), hop1_order(hop1_row), seed_row])
    sets = (second_count // seed_count, first_count // seed_count, 1)
    slots, requests = bucket_all(
        owners,
        rows,
        seed_count,
        sets,
        caps,
        (0, 0, caps[1]),
        (strides[0], strides[1], strides[1]),
        devices,
    )
    far_kinds = hop2_rel.reshape(seed_count, FAN1, FAN2).swapaxes(0, 1).reshape(-1, FAN2)
    edge_loss, mean_loss = fetch(
        requests,
        slots,
        features,
        w_first,
        w_second,
        (far_kinds, hop1_rel.reshape(seed_count, FAN1)),
        edge_mask[:, None],
        (caps[0], near_cap),
        strides,
        (second_count, first_count, seed_count),
        devices,
    )
    return (edge_loss[:, 0], mean_loss[0, 0])


def solution(mesh):
    placed = (
        P("dom", None),
        P(),
        P(),
        P("dom", None),
        P("dom"),
        P("dom", None),
        P("dom"),
        P("dom"),
        P("dom", None),
        P("dom"),
        P("dom"),
        P("dom"),
    )
    return jax.shard_map(
        shards, mesh=mesh, in_specs=placed, out_specs=(P("dom"), P()), check_vma=False
    )
```

```python
import functools

import jax
import jax.numpy as jnp
import numpy as np
from jax import lax
from jax.experimental import pallas as pl
from jax.experimental.pallas import tpu as pltpu
from jax.sharding import PartitionSpec as P

MESH = pl.DeviceIdType.MESH
HOP = 11
PIECE = 96
LANES = 128
LOADS = 8

R = 4
BLOCK = 128
NEG = 32
FAN1 = 4
FAN2 = 2


def round_up(value, multiple):
    return (value + multiple - 1) // multiple * multiple


def unroll_of(count):
    return max(step for step in range(1, 25) if count % step == 0)


def bucket_all(owners, rows, group, sets, caps, bases, strides, devices):
    blocks = owners.shape[0] // group
    onehot = owners[:, None] == jnp.arange(devices, dtype=jnp.int32)[None, :]
    hot = onehot.astype(jnp.bfloat16).reshape(blocks, group, devices)
    counter = jnp.arange(group, dtype=jnp.int32)
    earlier = (counter[:, None] > counter[None, :]).astype(jnp.bfloat16)
    prior = jnp.einsum("ij,bjd->bid", earlier, hot, preferred_element_type=jnp.float32)
    totals = jnp.sum(hot.astype(jnp.float32), axis=1)
    carry = []
    start = 0
    for count in sets:
        running = jnp.zeros((devices,), jnp.float32)
        for block in range(start, start + count):
            carry.append(running)
            running = running + totals[block]
        start += count
    prior = prior + jnp.stack(carry)[:, None, :]
    position = jnp.sum(prior * hot.astype(jnp.float32), axis=2).astype(jnp.int32)
    offsets = np.concatenate([[0], np.cumsum(caps)[:-1]])
    offset = jnp.asarray(np.repeat(offsets, sets), jnp.int32)
    base = jnp.asarray(np.repeat(np.asarray(bases), sets), jnp.int32)
    stride = jnp.asarray(np.repeat(np.asarray(strides), sets), jnp.int32)
    slots = owners.reshape(blocks, group) * stride[:, None] + base[:, None] + position
    place = (position + offset[:, None]).reshape(-1)
    width = round_up(sum(caps), LANES)
    placed = (place[:, None] == jnp.arange(width, dtype=jnp.int32)[None, :]).astype(jnp.bfloat16)
    high = jnp.where(onehot, (rows // 128)[:, None], 0).astype(jnp.bfloat16)
    low = jnp.where(onehot, (rows % 128)[:, None], 0).astype(jnp.bfloat16)
    digits = lax.dot_general(
        jnp.concatenate([high, low], axis=1),
        placed,
        (((0,), (0,)), ((), ())),
        preferred_element_type=jnp.float32,
    )
    requests = (digits[:devices] * 128.0 + digits[devices:]).astype(jnp.int32)
    return slots.reshape(-1), requests


def greet(devices, me):
    barrier = pltpu.get_barrier_semaphore()

    def hail(step, carry):
        other = lax.rem(me + step, devices)
        pl.semaphore_signal(barrier, inc=1, device_id=(other,), device_id_type=MESH)
        return carry

    lax.fori_loop(1, devices, hail, 0)
    pl.semaphore_wait(barrier, devices - 1)


def gather_rows(table, index_of, count, staging):
    step = unroll_of(count)

    def some(turn, carry):
        for lane in range(step):
            place = turn * step + lane
            staging[pl.ds(place, 1), :] = table[pl.ds(index_of(place), 1), :]
        return carry

    lax.fori_loop(0, count // step, some, 0)


def fetch_kernel(
    devices,
    caps,
    strides,
    counts,
    requests,
    slots,
    features,
    w_first,
    w_second,
    far_kinds,
    near_kinds,
    mask,
    loss_out,
    mean_out,
    table_half,
    table,
    arrived,
    wanted,
    far_send,
    near_send,
    far_recv,
    near_recv,
    far_table,
    near_table,
    staging,
    partial,
    near_rows,
    first_hop,
    first_seed,
    second,
    part,
    seen,
    load_sem,
    small_sem,
    ask_send,
    ask_recv,
    far_send_sem,
    far_recv_sem,
    near_send_sem,
    near_recv_sem,
    tell_send,
    tell_recv,
):
    me = lax.axis_index("dom")
    far_count, first_count, seed_count = counts
    width = table.shape[1]
    far_cap, near_cap = caps
    chunk = table.shape[0] // LOADS
    loads = []
    for turn in range(LOADS):
        where = pl.ds(turn * chunk, chunk)
        loads.append(
            pltpu.make_async_copy(features.at[where], table_half.at[where], load_sem.at[turn])
        )
        loads[-1].start()
    greet(devices, me)

    def ask(turn, carry):
        other = lax.rem(me + turn * HOP, devices)
        pltpu.make_async_remote_copy(
            src_ref=requests.at[other],
            dst_ref=arrived.at[me],
            send_sem=ask_send,
            recv_sem=ask_recv,
            device_id=(other,),
            device_id_type=MESH,
        ).start()
        return carry

    lax.fori_loop(1, devices, ask, 0)
    own = pltpu.make_async_copy(requests.at[me], arrived.at[me], small_sem)
    own.start()
    part_rows = chunk // 4
    for turn in range(LOADS):
        loads[turn].wait()

        def widen(quarter, carry):
            start = pl.multiple_of(turn * chunk + quarter * part_rows, part_rows)
            where = pl.ds(start, part_rows)
            table[where, :] = table_half[where, :].astype(jnp.float32)
            return carry

        lax.fori_loop(0, 4, widen, 0)
    own.wait()
    others = pl.ds(0, devices - 1)
    pltpu.make_async_copy(requests.at[others], arrived.at[others], ask_send).wait()
    pltpu.make_async_copy(requests.at[others], arrived.at[others], ask_recv).wait()
    move = pltpu.make_async_copy(arrived, wanted, small_sem)
    move.start()
    move.wait()

    def serve(first, cap, send, recv, send_sem, recv_sem):
        def pick(other):
            gather_rows(table, lambda place: wanted[other, 0, first + place], cap, staging)
            return staging[pl.ds(0, cap), :].astype(jnp.bfloat16)

        def one(turn, carry):
            other = lax.rem(me + turn * HOP, devices)
            send[other] = pick(other)
            pltpu.make_async_remote_copy(
                src_ref=send.at[other],
                dst_ref=recv.at[me],
                send_sem=send_sem,
                recv_sem=recv_sem,
                device_id=(other,),
                device_id_type=MESH,
            ).start()
            return carry

        lax.fori_loop(1, devices, one, 0)
        recv[me] = pick(me)

    serve(0, far_cap, far_send, far_recv, far_send_sem, far_recv_sem)
    serve(far_cap, near_cap, near_send, near_recv, near_send_sem, near_recv_sem)

    def settle(send, recv, recv_sem, cap, stride, wide):
        pltpu.make_async_copy(send.at[others], recv.at[others], recv_sem).wait()

        def spread(source, carry):
            where = pl.ds(pl.multiple_of(source * stride, 8), cap)
            wide[where, :] = recv[source].astype(jnp.float32)
            return carry

        lax.fori_loop(0, devices, spread, 0)

    def weighed(values, kinds, weights):
        fan = len(values)
        hot = [
            [(kinds[:, k : k + 1] == kind).astype(jnp.float32) for k in range(fan)]
            for kind in range(R)
        ]
        result = None
        for kind in range(R):
            share = 1.0 / jnp.maximum(sum(hot[kind][1:], hot[kind][0]), 1.0)
            mean = (hot[kind][0] * share) * values[0]
            for k in range(1, fan):
                mean = mean + (hot[kind][k] * share) * values[k]
            term = jnp.dot(
                mean.astype(jnp.bfloat16),
                weights[(kind + 1) * width : (kind + 2) * width, :],
                preferred_element_type=jnp.float32,
            )
            result = term if result is None else result + term
        return result

    def itself(values, weights):
        return jnp.dot(
            values.astype(jnp.bfloat16), weights[:width, :], preferred_element_type=jnp.float32
        )

    settle(far_send, far_recv, far_recv_sem, far_cap, strides[0], far_table)

    def far_piece(turn, carry):
        start = pl.multiple_of(turn * PIECE, PIECE)
        values = []
        for k in range(FAN2):
            gather_rows(
                far_table, lambda place: slots[k * first_count + start + place], PIECE, staging
            )
            values.append(staging[pl.ds(0, PIECE), :])
        where = pl.ds(start, PIECE)
        partial[where, :] = weighed(values, far_kinds[where, :], w_first)
        return carry

    lax.fori_loop(0, first_count // PIECE, far_piece, 0)
    settle(near_send, near_recv, near_recv_sem, near_cap, strides[1], near_table)
    gather_rows(
        near_table, lambda place: slots[far_count + place], first_count + seed_count, near_rows
    )

    def hop_piece(turn, carry):
        where = pl.ds(pl.multiple_of(turn * PIECE, PIECE), PIECE)
        layer = itself(near_rows[where, :], w_first) + partial[where, :]
        rounded = jnp.maximum(layer, 0.0).astype(jnp.bfloat16)
        first_hop[where, :] = rounded.astype(jnp.float32)
        return carry

    lax.fori_loop(0, first_count // PIECE, hop_piece, 0)

    def seed_layer(start, own_rows, own_start, rows, weights):
        where = pl.ds(start, PIECE)
        values = [
            rows[pl.ds(pl.multiple_of(k * seed_count + start, PIECE), PIECE), :]
            for k in range(FAN1)
        ]
        own_where = pl.ds(pl.multiple_of(own_start + start, PIECE), PIECE)
        return itself(own_rows[own_where, :], weights) + weighed(
            values, near_kinds[where, :], weights
        )

    def seed_piece(turn, carry):
        start = pl.multiple_of(turn * PIECE, PIECE)
        where = pl.ds(start, PIECE)
        layer = seed_layer(start, near_rows, first_count, near_rows, w_first)
        first_seed[where, :] = jnp.maximum(layer, 0.0).astype(jnp.bfloat16).astype(jnp.float32)
        second[where, :] = seed_layer(start, first_seed, 0, first_hop, w_second)
        return carry

    lax.fori_loop(0, seed_count // PIECE, seed_piece, 0)

    blocks = mask.shape[0]
    positives = blocks * BLOCK
    loss_sum = jnp.zeros((1, 1), jnp.float32)
    edge_sum = jnp.zeros((1, 1), jnp.float32)

    def pairs(left, right):
        return lax.dot_general(
            left,
            right,
            (((1,), (1,)), ((), ())),
            precision=lax.Precision.HIGHEST,
            preferred_element_type=jnp.float32,
        )

    for block in range(blocks):
        sources = second[block * BLOCK : (block + 1) * BLOCK, :]
        targets = second[positives + block * BLOCK : positives + (block + 1) * BLOCK, :]
        first_neg = 2 * positives + block * NEG
        negatives = second[first_neg : first_neg + NEG, :]
        positive = pairs(jnp.ones((8, width), jnp.float32), sources * targets)[0:1, :]
        negative = pairs(negatives, sources)
        top_score = jnp.maximum(positive, jnp.max(negative, axis=0, keepdims=True))
        spread_sum = jnp.exp(positive - top_score) + jnp.sum(
            jnp.exp(negative - top_score), axis=0, keepdims=True
        )
        edge_loss = top_score + jnp.log(spread_sum) - positive
        loss_out[block : block + 1, :] = edge_loss
        counted = mask[block : block + 1, :].astype(jnp.float32)
        loss_sum = loss_sum + jnp.sum(counted * edge_loss, axis=1, keepdims=True)
        edge_sum = edge_sum + jnp.sum(counted, axis=1, keepdims=True)
    lane = lax.broadcasted_iota(jnp.int32, (1, LANES), 1)
    part[...] = jnp.where(lane == 0, loss_sum, jnp.where(lane == 1, edge_sum, 0.0))

    def tell(turn, carry):
        other = lax.rem(me + turn * HOP, devices)
        pltpu.make_async_remote_copy(
            src_ref=part,
            dst_ref=seen.at[me],
            send_sem=tell_send,
            recv_sem=tell_recv,
            device_id=(other,),
            device_id_type=MESH,
        ).start()
        return carry

    lax.fori_loop(1, devices, tell, 0)
    seen[me] = part[...]
    pltpu.make_async_copy(far_send.at[others], far_recv.at[others], far_send_sem).wait()
    pltpu.make_async_copy(near_send.at[others], near_recv.at[others], near_send_sem).wait()
    pltpu.make_async_copy(seen.at[others], seen.at[others], tell_recv).wait()
    pltpu.make_async_copy(seen.at[others], seen.at[others], tell_send).wait()
    total = jnp.sum(seen[...], axis=0)
    mean_out[...] = total[:, 0:1] / jnp.maximum(total[:, 1:2], 1.0)


def fetch(
    requests, slots, features, w_first, w_second, kinds, mask, caps, strides, counts, devices
):
    nodes, width = features.shape
    far_cap, near_cap = caps
    asked = requests.shape[1]
    half, full = jnp.bfloat16, jnp.float32
    vmem = pl.BlockSpec(memory_space=pltpu.VMEM)
    return pl.pallas_call(
        functools.partial(fetch_kernel, devices, caps, strides, counts),
        out_shape=[
            jax.ShapeDtypeStruct(mask.shape, full),
            jax.ShapeDtypeStruct((1, 1), full),
        ],
        in_specs=[
            vmem,
            pl.BlockSpec(memory_space=pltpu.SMEM),
            pl.BlockSpec(memory_space=pl.ANY),
        ]
        + [vmem] * 5,
        out_specs=[vmem, vmem],
        scratch_shapes=[
            pltpu.VMEM((nodes, width), half),
            pltpu.VMEM((nodes, width), full),
            pltpu.VMEM((devices, 1, asked), jnp.int32),
            pltpu.SMEM((devices, 1, asked), jnp.int32),
            pltpu.VMEM((devices, far_cap, width), half),
            pltpu.VMEM((devices, near_cap, width), half),
            pltpu.VMEM((devices, far_cap, width), half),
            pltpu.VMEM((devices, near_cap, width), half),
            pltpu.VMEM((devices * strides[0], width), full),
            pltpu.VMEM((devices * strides[1], width), full),
            pltpu.VMEM((round_up(max(far_cap, near_cap, PIECE), 8), width), full),
            pltpu.VMEM((counts[1], width), full),
            pltpu.VMEM((counts[1] + counts[2], width), full),
            pltpu.VMEM((counts[1], width), full),
            pltpu.VMEM((counts[2], width), full),
            pltpu.VMEM((counts[2], width), full),
            pltpu.VMEM((1, LANES), full),
            pltpu.VMEM((devices, 1, LANES), full),
        ]
        + [pltpu.SemaphoreType.DMA((LOADS,))]
        + [pltpu.SemaphoreType.DMA(())] * 9,
        compiler_params=pltpu.CompilerParams(
            collective_id=0, has_side_effects=True, vmem_limit_bytes=60 * 1024 * 1024
        ),
        name="fetch",
    )(
        requests.reshape(devices, 1, asked),
        slots,
        features,
        w_first,
        w_second,
        kinds[0],
        kinds[1],
        mask,
    )


def shards(
    features,
    w_first,
    w_second,
    seed_owner,
    seed_row,
    hop1_owner,
    hop1_row,
    hop1_rel,
    hop2_owner,
    hop2_row,
    hop2_rel,
    edge_mask,
):
    devices = lax.axis_size("dom")
    seed_count = seed_row.shape[0]
    first_count = hop1_row.shape[0]
    second_count = hop2_row.shape[0]
    caps = [
        (2 * length + devices - 1) // devices for length in (second_count, first_count, seed_count)
    ]
    near_cap = caps[1] + caps[2]
    strides = (round_up(caps[0], 8), round_up(near_cap, 8))

    def turned(values, fan):
        return values.reshape(-1, fan).T

    def hop2_order(values):
        return turned(values, FAN2).reshape(FAN2, seed_count, FAN1).swapaxes(1, 2).reshape(-1)

    def hop1_order(values):
        return turned(values, FAN1).reshape(-1)

    owners = jnp.concatenate(
        [hop2_order(hop2_owner[:, 0]), hop1_order(hop1_owner[:, 0]), seed_owner[:, 0]]
    )
    rows = jnp.concatenate([hop2_order(hop2_row), hop1_order(hop1_row), seed_row])
    sets = (second_count // seed_count, first_count // seed_count, 1)
    slots, requests = bucket_all(
        owners,
        rows,
        seed_count,
        sets,
        caps,
        (0, 0, caps[1]),
        (strides[0], strides[1], strides[1]),
        devices,
    )
    far_kinds = hop2_rel.reshape(seed_count, FAN1, FAN2).swapaxes(0, 1).reshape(-1, FAN2)
    edge_loss, mean_loss = fetch(
        requests,
        slots,
        features,
        w_first,
        w_second,
        (far_kinds, hop1_rel.reshape(seed_count, FAN1)),
        edge_mask.reshape(-1, BLOCK),
        (caps[0], near_cap),
        strides,
        (second_count, first_count, seed_count),
        devices,
    )
    return (edge_loss.reshape(-1), mean_loss[0, 0])


def solution(mesh):
    placed = (
        P("dom", None),
        P(),
        P(),
        P("dom", None),
        P("dom"),
        P("dom", None),
        P("dom"),
        P("dom"),
        P("dom", None),
        P("dom"),
        P("dom"),
        P("dom"),
    )
    return jax.shard_map(
        shards, mesh=mesh, in_specs=placed, out_specs=(P("dom"), P()), check_vma=False
    )
```
